512 devices in a mesh: rep: 32 (over x_lo, z, core), tp: 16 (over y, x_hi).
Axes of the slice: x: 4 (x_hi: 2, x_lo: 2; x = x_hi * 2 + x_lo), y: 8, z: 8, core: 2. Of those that a mesh axis runs over, the one named last changes fastest.
Arguments:
- queries: bfloat16 [256, 8192], P('rep', 'tp'), may hold values from -200 to 200
- new_keys: bfloat16 [256, 1024], P('rep', 'tp'), may hold values from -6 to 6
- new_values: bfloat16 [256, 1024], P('rep', 'tp'), may hold values from -6 to 6
- key_pool: bfloat16 [3072, 128, 1024], P('rep', 'tp'), may hold values from -6 to 6
- value_pool: bfloat16 [3072, 128, 1024], P('rep', 'tp'), may hold values from -6 to 6
- lengths: int32 [256], replicated, may hold values from 1 to 1536, as said below
- page_table: int32 [256, 12], P('rep'), may hold values from -1 to 95, as said below
- mig_slot: int32 [32], replicated, may hold values from 0 to 7
- mig_dst: int32 [32], replicated, may hold values from 0 to 31, as said below
Outputs:
- attended: bfloat16 [256, 8192], P('rep', 'tp')
- moved_keys: bfloat16 [384, 128, 1024], P('rep', 'tp')
- moved_values: bfloat16 [384, 128, 1024], P('rep', 'tp')
The draws below stay inside these ranges and needn't reach their ends.
Inputs may be any that keep to these rules, and one draw needn't show every extreme that they name: mig_dst[r] = (r + c) mod 32 for one offset c with 1 <= c < 32, the same for every replica. `page_table`: row q lists distinct pool pages of its replica for its first ceil(lengths[q] / 128) pages and -1 after them. `lengths`: some request has exactly 1536 cached tokens.
All inputs are finite; a program needn't handle non-finite values.
Results may differ from the reference program's by a relative error of at most 0.0065.
Values may be sent and summed in bfloat16 or wider, within the bound.
A program may use at most 64 MiB of HBM per device.

```python
import math
import jax
import jax.numpy as jnp
from jax import lax

H = 64
KVH = 8
DH = 128
PAGE = 128
PAGES_REQ = 12
REQ_REP = 8
REPLICAS = 32
REQS = 256
POOL = 96
N_REP = 32


def live_lengths(key):
    drawn = jax.random.randint(jax.random.fold_in(key, 101), (REQS,), 1, PAGES_REQ * PAGE + 1)
    return drawn.at[0].set(PAGES_REQ * PAGE).astype(jnp.int32)


def draw_lengths(key, part):
    return live_lengths(key)


def draw_page_table(key, part):
    cached = live_lengths(key)
    page_count = (cached + PAGE - 1) // PAGE
    replica_keys = jax.random.split(jax.random.fold_in(key, 202), REPLICAS)
    orders = jax.vmap(lambda subkey: jax.random.permutation(subkey, POOL))(replica_keys)
    tables = orders.reshape(REQS, PAGES_REQ).astype(jnp.int32)
    columns = jnp.arange(PAGES_REQ, dtype=jnp.int32)
    return jnp.where(columns[None, :] < page_count[:, None], tables, -1).astype(jnp.int32)


def draw_mig_dst(key, part):
    stride = jax.random.randint(jax.random.fold_in(key, 303), (), 1, REPLICAS)
    return ((jnp.arange(REPLICAS, dtype=jnp.int32) + stride) % REPLICAS).astype(jnp.int32)


def draw_queries(key, part):
    base = jnp.clip(jax.random.normal(key, (REQS, H * DH), jnp.float32), -5.0, 5.0)
    base = base * 1.5
    return base.astype(jnp.bfloat16)


def with_ends(result, key, least, top_value):
    extent = result.shape
    spot = [jax.random.randint(jax.random.fold_in(key, axis), (), 0, extent[axis]) for axis in range(len(extent))]
    result = result.at[tuple(spot)].set(least)
    longest = extent.index(max(extent))
    spot[longest] = (spot[longest] + 1) % extent[longest]
    return result.at[tuple(spot)].set(top_value)


def levels(key, shape, cuts, low, top_value):
    gain, own = 1.0, jax.random.fold_in(key, 6)
    for position, parts in cuts:
        draws = jnp.exp(jax.random.uniform(jax.random.fold_in(own, position), (parts,), jnp.float32, low / len(cuts), top_value / len(cuts)))
        gain = gain * jnp.repeat(draws, shape[position] // parts).reshape([-1 if axis == position else 1 for axis in range(len(shape))])
    return gain


def scatter_about(key, shape, spread, most, shards=(), kind=jnp.bfloat16):
    values = spread * jax.random.normal(key, shape, jnp.float32)
    if shards:
        values = values * levels(key, shape, shards, -0.22, 0.18)
    return jnp.clip(values, -most, most).astype(kind)


def setup_inputs(seed: int = 0) -> dict:
    keys = jax.random.split(jax.random.key(seed), 10)
    return {
        "queries": draw_queries(jax.random.fold_in(keys[9], 71), 0),
        "new_keys": scatter_about(keys[1], (REQS, KVH * DH), 1.5, 6.0, ((0, 32), (1, 16))),
        "new_values": scatter_about(keys[2], (REQS, KVH * DH), 1.0, 6.0, ((0, 32), (1, 16))),
        "key_pool": scatter_about(keys[3], (N_REP * POOL, PAGE, KVH * DH), 1.0, 6.0, ((0, 32), (1, 16))),
        "value_pool": scatter_about(keys[4], (N_REP * POOL, PAGE, KVH * DH), 1.0, 6.0, ((0, 32), (1, 16))),
        "lengths": draw_lengths(jax.random.fold_in(keys[9], 71), 0),
        "page_table": draw_page_table(jax.random.fold_in(keys[9], 71), 0),
        "mig_slot": with_ends(jax.random.randint(keys[7], (REPLICAS,), 0, REQ_REP), jax.random.fold_in(keys[7], 1), 0, REQ_REP - 1).astype(jnp.int32),
        "mig_dst": draw_mig_dst(jax.random.fold_in(keys[9], 71), 0),
    }


def reference(queries, new_keys, new_values, key_pool, value_pool, lengths, page_table, mig_slot, mig_dst):
    replica_ids = jnp.arange(N_REP, dtype=jnp.int32)
    scaling = 1.0 / math.sqrt(DH)

    def one_replica(replica):
        source = jnp.sum(jnp.where(mig_dst == replica, replica_ids, 0)).astype(jnp.int32)
        leaving = mig_slot[replica]
        arriving = (source * REQ_REP + mig_slot[source]).astype(jnp.int32)
        slot_ids = jnp.arange(REQ_REP, dtype=jnp.int32)
        owner_rep = jnp.where(slot_ids == leaving, source, replica).astype(jnp.int32)
        owner_req = jnp.where(slot_ids == leaving, arriving, replica * REQ_REP + slot_ids).astype(jnp.int32)
        table_rows = page_table[owner_req]
        page_index = (owner_rep[:, None] * POOL + jnp.maximum(table_rows, 0)).astype(jnp.int32)
        cached_keys = key_pool[page_index].reshape(REQ_REP, PAGES_REQ * PAGE, KVH, DH).astype(jnp.float32)
        cached_values = value_pool[page_index].reshape(REQ_REP, PAGES_REQ * PAGE, KVH, DH).astype(jnp.float32)
        live_len = lengths[owner_req]
        positions = jnp.arange(PAGES_REQ * PAGE, dtype=jnp.int32)
        usable = positions[None, :] < live_len[:, None]
        start = (replica * REQ_REP).astype(jnp.int32)
        query_rows = lax.dynamic_slice_in_dim(queries, start, REQ_REP, 0).reshape(REQ_REP, KVH, H // KVH, DH).astype(jnp.float32)
        fresh_keys = lax.dynamic_slice_in_dim(new_keys, start, REQ_REP, 0).reshape(REQ_REP, KVH, DH).astype(jnp.float32)
        fresh_values = lax.dynamic_slice_in_dim(new_values, start, REQ_REP, 0).reshape(REQ_REP, KVH, DH).astype(jnp.float32)
        scores = jnp.einsum('rgqd,rngd->rgqn', query_rows, cached_keys) * scaling
        new_score = jnp.einsum('rgqd,rgd->rgq', query_rows, fresh_keys) * scaling
        masked = jnp.where(usable[:, None, None, :], scores, -jnp.inf)
        maxima = jnp.maximum(masked.max(-1), new_score)
        weights = jnp.where(usable[:, None, None, :], jnp.exp(masked - maxima[..., None]), 0.0)
        new_weight = jnp.exp(new_score - maxima)
        totals = weights.sum(-1) + new_weight
        rounded = lax.optimization_barrier(weights.astype(jnp.bfloat16)).astype(jnp.float32)
        rounded_new = lax.optimization_barrier(new_weight.astype(jnp.bfloat16)).astype(jnp.float32)
        mixed = jnp.einsum('rgqn,rngd->rgqd', rounded, cached_values)
        mixed = mixed + rounded_new[..., None] * fresh_values[:, :, None, :]
        attended = (mixed / totals[..., None]).reshape(REQ_REP, H * DH).astype(jnp.bfloat16)
        moved_rows = page_table[arriving]
        moved_index = (source * POOL + jnp.maximum(moved_rows, 0)).astype(jnp.int32)
        present = (moved_rows >= 0)[:, None, None]
        moved_keys = jnp.where(present, key_pool[moved_index], jnp.zeros((), jnp.bfloat16))
        moved_values = jnp.where(present, value_pool[moved_index], jnp.zeros((), jnp.bfloat16))
        return (attended, moved_keys, moved_values)
    attended, moved_keys, moved_values = lax.map(one_replica, replica_ids)
    return (attended.reshape(N_REP * REQ_REP, H * DH), moved_keys.reshape(N_REP * PAGES_REQ, PAGE, KVH * DH), moved_values.reshape(N_REP * PAGES_REQ, PAGE, KVH * DH))
```

```python
import functools
import math

import jax
import jax.numpy as jnp
from jax import lax
from jax.experimental import pallas as pl
from jax.experimental.pallas import tpu as pltpu
from jax.sharding import PartitionSpec as P

H = 64
KVH = 8
DH = 128
PAGE = 128
GROUP = H // KVH
NEG = -1e30
MESH = pl.DeviceIdType.MESH


def kernel(
    shift,
    len_s, pt_s, slot_s, pt_v, q_h, nk_h, nv_h, kp_h, vp_h,
    att_ref, mk_ref, mv_ref,
    kbuf, vbuf, qall, qmv, qsel, nkb, nvb, pbuf, lim_ref,
    osend, orecv, ssend, srecv, rsend, rrecv,
    loc_sem, q_snd, q_rcv, mq_snd, mq_rcv, n_snd, n_rcv, o_snd, o_rcv, s_snd, s_rcv,
    p_snd, p_rcv, x_snd, x_rcv,
):
    f32, bf16 = jnp.float32, jnp.bfloat16
    reps, tps = lax.axis_size("rep"), lax.axis_size("tp")
    rep, me = lax.axis_index("rep"), lax.axis_index("tp")
    slots, pages_most = pt_s.shape
    pool, rows, width = kbuf.shape
    tokens = pool * rows
    heads = H // tps
    per_group = tps // KVH
    my_group = me // per_group
    scaling = 1.0 / math.sqrt(DH)
    ahead = lax.rem(rep + shift, reps)
    behind = lax.rem(rep + reps - shift, reps)
    mate = me + 1 - 2 * lax.rem(me, 2)

    def peer(i):
        return lax.rem(me + i, tps)

    def to_tp(src, dst, snd, rcv, t):
        return pltpu.make_async_remote_copy(
            src_ref=src, dst_ref=dst, send_sem=snd, recv_sem=rcv,
            device_id=(rep, t), device_id_type=MESH,
        )

    def to_rep(src, dst, snd, rcv, r):
        return pltpu.make_async_remote_copy(
            src_ref=src, dst_ref=dst, send_sem=snd, recv_sem=rcv,
            device_id=(r, me), device_id_type=MESH,
        )

    load_q = pltpu.make_async_copy(q_h, qall.at[me], loc_sem.at[0])
    load_k = pltpu.make_async_copy(kp_h, kbuf, loc_sem.at[1])
    load_v = pltpu.make_async_copy(vp_h, vbuf, loc_sem.at[2])
    load_nk = pltpu.make_async_copy(nk_h, nkb.at[lax.rem(me, 2)], loc_sem.at[3])
    load_nv = pltpu.make_async_copy(nv_h, nvb.at[lax.rem(me, 2)], loc_sem.at[4])
    load_q.start()
    load_k.start()
    load_v.start()
    load_nk.start()
    load_nv.start()

    barrier = pltpu.get_barrier_semaphore()

    def greet(i, _):
        pl.semaphore_signal(barrier, inc=1, device_id=(rep, peer(i)), device_id_type=MESH)
        return 0

    for r in (ahead, behind):
        pl.semaphore_signal(barrier, inc=1, device_id=(r, me), device_id_type=MESH)
    lax.fori_loop(1, tps, greet, 0)

    leaving = slot_s[rep]
    slot_ids = lax.broadcasted_iota(jnp.int32, (slots, DH), 0)
    lane_ids = lax.broadcasted_iota(jnp.int32, (slots, DH), 1)
    is_moving = slot_ids == leaving

    load_q.wait()
    for h in range(heads):
        part = qall[me, :, h * DH : (h + 1) * DH].astype(f32)
        qsel[:, h * DH : (h + 1) * DH] = jnp.sum(
            jnp.where(is_moving, part, 0.0), axis=0, keepdims=True
        )
    load_nk.wait()
    load_nv.wait()
    for load, buf, base in ((load_k, kbuf, 0), (load_v, vbuf, pages_most)):
        load.wait()

        def take(j, _):
            page = pt_s[leaving, j]
            rows_in = buf[jnp.maximum(page, 0)]
            pbuf[base + j] = jnp.where(page >= 0, rows_in, jnp.zeros((), bf16))
            return 0

        lax.fori_loop(0, pages_most, take, 0)

    pl.semaphore_wait(barrier, tps + 1)

    ask = to_rep(qsel, qmv.at[me], x_snd.at[0], x_rcv.at[0], behind)
    ask.start()
    move_k = to_rep(pbuf.at[pl.ds(0, pages_most)], mk_ref, p_snd.at[0], p_rcv.at[0], ahead)
    move_v = to_rep(pbuf.at[pl.ds(pages_most, pages_most)], mv_ref, p_snd.at[1], p_rcv.at[1], ahead)
    move_k.start()
    move_v.start()

    def q_copy(t, slot):
        return to_tp(qall.at[me], qall.at[me], q_snd.at[t], q_rcv.at[me], t)

    def mq_copy(t, slot):
        return to_tp(qmv.at[me], qmv.at[me], mq_snd.at[t], mq_rcv.at[me], t)

    def send_q(i, _):
        t = peer(i)
        to_tp(qall.at[me], qall.at[me], q_snd.at[t], q_rcv.at[me], t).start()
        return 0

    lax.fori_loop(1, tps, send_q, 0)
    half = lax.rem(me, 2)
    give_nk = to_tp(nkb.at[half], nkb.at[half], n_snd.at[0], n_rcv.at[0], mate)
    give_nv = to_tp(nvb.at[half], nvb.at[half], n_snd.at[1], n_rcv.at[1], mate)
    give_nk.start()
    give_nv.start()

    lens = jnp.zeros((slots, DH), jnp.int32)
    for i in range(slots):
        lens = jnp.where(slot_ids == i, len_s[rep * slots + i], lens)
    table = pt_v[...]
    for b in range(tokens // DH):
        token = lane_ids + b * DH
        page_of = lax.shift_right_logical(token, 3)
        left = jnp.zeros((slots, DH), jnp.int32)
        for j in range(pages_most):
            left = jnp.where(table[:, j : j + 1] == page_of, lens - j * PAGE, left)
        row = jnp.bitwise_and(token, rows - 1) + me * rows
        lim_ref[:, b * DH : (b + 1) * DH] = jnp.where(left > row, 1.0, 0.0)

    ask.wait_recv()

    def send_mq(i, _):
        t = peer(i)
        to_tp(qmv.at[me], qmv.at[me], mq_snd.at[t], mq_rcv.at[me], t).start()
        return 0

    lax.fori_loop(1, tps, send_mq, 0)

    def arrived_q(i, _):
        t = peer(i)
        to_tp(qall.at[t], qall.at[t], q_snd.at[t], q_rcv.at[t], t).wait_recv()
        return 0

    def arrived_mq(i, _):
        t = peer(i)
        to_tp(qmv.at[t], qmv.at[t], mq_snd.at[t], mq_rcv.at[t], t).wait_recv()
        return 0

    lax.fori_loop(1, tps, arrived_q, 0)
    lax.fori_loop(1, tps, arrived_mq, 0)

    def group_at(k):
        odd = lax.rem(k, 2)
        off = KVH // 2 + (1 - odd) * (k // 2) - odd * ((k + 1) // 2)
        return lax.rem(my_group + off, KVH)

    def send_parts(k):
        for j in range(per_group):
            t = group_at(k) * per_group + j

            @pl.when(t != me)
            def _():
                to_tp(osend.at[t], orecv.at[me], o_snd.at[t], o_rcv.at[me], t).start()
                to_tp(ssend.at[t], srecv.at[me], s_snd.at[t], s_rcv.at[me], t).start()

    def attend(k, _):
        g = group_at(k)
        pieces = []
        for j in range(per_group):
            t = g * per_group + j
            for h in range(heads):
                own = qall[t, :, h * DH : (h + 1) * DH].astype(f32)
                moved = qmv[t, :, h * DH : (h + 1) * DH]
                pieces.append(jnp.where(is_moving, jnp.broadcast_to(moved, own.shape), own))
        query = jnp.concatenate(pieces, axis=0).astype(bf16)
        col = pl.multiple_of(g * DH, DH)
        keys = kbuf[:, :, pl.ds(col, DH)].reshape(tokens, DH)
        values = vbuf[:, :, pl.ds(col, DH)].reshape(tokens, DH)
        s = lax.dot_general(
            query, keys, (((1,), (1,)), ((), ())), preferred_element_type=f32
        ).reshape(GROUP, slots, tokens)
        usable = (lim_ref[...] > 0.5)[None]
        s = jnp.where(usable, s * scaling, NEG)
        m = jnp.max(s, axis=-1, keepdims=True)
        p = jnp.where(usable, jnp.exp(s - m), 0.0)
        total = jnp.sum(p, axis=-1, keepdims=True)
        o = lax.dot_general(
            p.reshape(GROUP * slots, tokens).astype(bf16), values,
            (((1,), (0,)), ((), ())), preferred_element_type=f32,
        )
        for j in range(per_group):
            t = g * per_group + j
            osend[t] = o[j * heads * slots : (j + 1) * heads * slots].astype(bf16)
            stats = jnp.zeros((slots, DH), f32)
            for h in range(heads):
                stats = jnp.where(lane_ids == h, m[j * heads + h], stats)
                stats = jnp.where(lane_ids == heads + h, total[j * heads + h], stats)
            ssend[t] = stats

        @pl.when(k > 0)
        def _():
            send_parts(k - 1)

        return 0

    lax.fori_loop(0, KVH, attend, 0)
    orecv[me] = osend[me]
    srecv[me] = ssend[me]

    give_nk.wait_recv()
    give_nv.wait_recv()
    send_parts(KVH - 1)
    at_row = lax.broadcasted_iota(jnp.int32, (DH // 2, DH), 0)
    at_col = lax.broadcasted_iota(jnp.int32, (DH // 2, DH), 1)
    fresh = []
    for buf in (nkb, nvb):
        both = jnp.zeros((slots, DH), f32)
        for i in range(2):
            place = jnp.where(at_col == at_row + i * (DH // 2), 1.0, 0.0).astype(bf16)
            both = both + jnp.dot(buf[i], place, preferred_element_type=f32)
        fresh.append(both)
    new_key, new_value = fresh
    new_scores = []
    for h in range(heads):
        own = qall[me, :, h * DH : (h + 1) * DH].astype(f32)
        new_scores.append(jnp.sum(own * new_key, axis=-1, keepdims=True) * scaling)

    def arrived_parts(i, _):
        t = peer(i)
        to_tp(osend.at[t], orecv.at[t], o_snd.at[t], o_rcv.at[t], t).wait_recv()
        to_tp(ssend.at[t], srecv.at[t], s_snd.at[t], s_rcv.at[t], t).wait_recv()
        return 0

    lax.fori_loop(1, tps, arrived_parts, 0)

    peak = srecv[0]
    for t in range(1, tps):
        peak = jnp.maximum(peak, srecv[t])
    total = jnp.zeros((slots, DH), f32)
    mixed = [jnp.zeros((slots, DH), f32) for _ in range(heads)]
    for t in range(tps):
        stats = srecv[t]
        factor = jnp.exp(stats - peak)
        total = total + factor * pltpu.roll(stats, DH - heads, 1)
        part = orecv[t].astype(f32)
        for h in range(heads):
            mixed[h] = mixed[h] + factor[:, h : h + 1] * part[h * slots : (h + 1) * slots]

    for h in range(heads):
        rsend[h] = jnp.sum(jnp.where(is_moving, mixed[h], 0.0), axis=0, keepdims=True)
    rsend[heads] = jnp.sum(jnp.where(is_moving, peak, 0.0), axis=0, keepdims=True)
    rsend[heads + 1] = jnp.sum(jnp.where(is_moving, total, 0.0), axis=0, keepdims=True)
    answer = to_rep(rsend, rrecv, x_snd.at[1], x_rcv.at[1], ahead)
    answer.start()
    answer.wait_recv()
    peak = jnp.where(is_moving, jnp.broadcast_to(rrecv[heads], peak.shape), peak)
    total = jnp.where(is_moving, jnp.broadcast_to(rrecv[heads + 1], total.shape), total)
    for h in range(heads):
        mix = jnp.where(is_moving, jnp.broadcast_to(rrecv[h], (slots, DH)), mixed[h])
        old_peak = peak[:, h : h + 1]
        new_score = new_scores[h]
        top = jnp.maximum(old_peak, new_score)
        old_scale = jnp.exp(old_peak - top)
        new_weight = jnp.exp(new_score - top)
        denominator = total[:, h : h + 1] * old_scale + new_weight
        rounded = new_weight.astype(bf16).astype(f32)
        out = (mix * old_scale + rounded * new_value) / denominator
        att_ref[:, h * DH : (h + 1) * DH] = out.astype(bf16)

    ask.wait_send()
    answer.wait_send()
    give_nk.wait_send()
    give_nv.wait_send()

    def sent(i, _):
        t = peer(i)
        to_tp(qall.at[me], qall.at[me], q_snd.at[t], q_rcv.at[me], t).wait_send()
        to_tp(qmv.at[me], qmv.at[me], mq_snd.at[t], mq_rcv.at[me], t).wait_send()
        to_tp(osend.at[t], orecv.at[me], o_snd.at[t], o_rcv.at[me], t).wait_send()
        to_tp(ssend.at[t], srecv.at[me], s_snd.at[t], s_rcv.at[me], t).wait_send()
        return 0

    lax.fori_loop(1, tps, sent, 0)
    move_k.wait()
    move_v.wait()


def call_for(shift, tps, slots, pages_most, pool, rows, width, columns):
    f32, bf16 = jnp.float32, jnp.bfloat16
    heads = H // tps
    vmem = pl.BlockSpec(memory_space=pltpu.VMEM)
    smem = pl.BlockSpec(memory_space=pltpu.SMEM)
    hbm = pl.BlockSpec(memory_space=pl.ANY)
    dma = pltpu.SemaphoreType.DMA
    moved = jax.ShapeDtypeStruct((pages_most, rows, width), bf16)
    return pl.pallas_call(
        functools.partial(kernel, shift),
        out_shape=(jax.ShapeDtypeStruct((slots, columns), bf16), moved, moved),
        in_specs=[smem, smem, smem, vmem, hbm, hbm, hbm, hbm, hbm],
        out_specs=(vmem, hbm, hbm),
        scratch_shapes=[
            pltpu.VMEM((pool, rows, width), bf16),
            pltpu.VMEM((pool, rows, width), bf16),
            pltpu.VMEM((tps, slots, columns), bf16),
            pltpu.VMEM((tps, 1, columns), f32),
            pltpu.VMEM((1, columns), f32),
            pltpu.VMEM((2, slots, DH // 2), bf16),
            pltpu.VMEM((2, slots, DH // 2), bf16),
            pltpu.VMEM((2 * pages_most, rows, width), bf16),
            pltpu.VMEM((slots, pool * rows), f32),
            pltpu.VMEM((tps, heads * slots, DH), bf16),
            pltpu.VMEM((tps, heads * slots, DH), bf16),
            pltpu.VMEM((tps, slots, DH), f32),
            pltpu.VMEM((tps, slots, DH), f32),
            pltpu.VMEM((heads + 2, 1, DH), f32),
            pltpu.VMEM((heads + 2, 1, DH), f32),
            dma((5,)),
            dma((tps,)), dma((tps,)),
            dma((tps,)), dma((tps,)),
            dma((2,)), dma((2,)),
            dma((tps,)), dma((tps,)),
            dma((tps,)), dma((tps,)),
            dma((2,)), dma((2,)),
            dma((2,)), dma((2,)),
        ],
        compiler_params=pltpu.CompilerParams(
            collective_id=shift, has_side_effects=True,
        ),
        name="serve_%d" % shift,
    )


ONLY = None


def body(
    queries, new_keys, new_values, key_pool, value_pool, lengths, page_table, mig_slot, mig_dst
):
    replicas, tps = lax.axis_size("rep"), lax.axis_size("tp")
    slots, pages_most = page_table.shape
    sizes = (tps, slots, pages_most, *key_pool.shape, queries.shape[1])
    operands = (
        lengths, page_table, mig_slot, page_table,
        queries, new_keys, new_values, key_pool, value_pool,
    )
    if ONLY is not None:
        return call_for(ONLY, *sizes)(*operands)
    return lax.switch(
        mig_dst[0] - 1,
        [call_for(shift, *sizes) for shift in range(1, replicas)],
        *operands,
    )


def solution(mesh):
    placed = (
        P("rep", "tp"),
        P("rep", "tp"),
        P("rep", "tp"),
        P("rep", "tp", None),
        P("rep", "tp", None),
        P(),
        P("rep", None),
        P(),
        P(),
    )
    return jax.shard_map(
        body,
        mesh=mesh,
        in_specs=placed,
        out_specs=(P("rep", "tp"), P("rep", "tp", None), P("rep", "tp", None)),
        check_vma=False,
    )
```

```python
import functools
import math

import jax
import jax.numpy as jnp
from jax import lax
from jax.experimental import pallas as pl
from jax.experimental.pallas import tpu as pltpu
from jax.sharding import PartitionSpec as P

H = 64
KVH = 8
DH = 128
PAGE = 128
GROUP = H // KVH
NEG = -1e30
LOW = -1e29
UNROLL = 2
MESH = pl.DeviceIdType.MESH
CHUNKS = 2


def plan(shift):
    return {
        6: ((-2, 16, 8),),
        7: ((1, 0, 12), (-2, 12, 12)),
        8: ((1, 0, 12), (-1, 12, 12)),
        9: ((-1, 0, 12), (2, 12, 12)),
        10: ((2, 16, 8),),
    }.get(shift % 16, ())


def finish(att, mk, mv, att_out, mk_out, mv_out, sem):
    copies = [
        pltpu.make_async_copy(src, dst, sem.at[i])
        for i, (src, dst) in enumerate(((mk, mk_out), (mv, mv_out), (att, att_out)))
    ]
    for copy in copies:
        copy.start()
    for copy in copies:
        copy.wait()


def kernel(
    shift,
    len_h, pt_h, slot_h, q_h, nk_h, nv_h, kp_h, vp_h,
    att_ref, mk_ref, mv_ref,
    len_s, pt_s, slot_s, pt_v, kbuf, vbuf, qall, qmv, qsel, nkb, nvb, pbuf, lim_ref,
    osend, orecv, ssend, srecv, rsend, rrecv, hold,
    loc_sem, q_snd, q_rcv, mq_snd, mq_rcv, n_snd, n_rcv, o_snd, o_rcv, s_snd, s_rcv,
    p_snd, p_rcv, x_snd, x_rcv, h_snd, h_rcv, f_snd, f_rcv,
):
    f32, bf16 = jnp.float32, jnp.bfloat16
    reps, tps = lax.axis_size("rep"), lax.axis_size("tp")
    rep, me = lax.axis_index("rep"), lax.axis_index("tp")
    slots, pages_most = pt_s.shape
    pool, rows, width = kp_h.shape
    tokens = pool * rows
    heads = H // tps
    per_group = tps // KVH
    my_group = me // per_group
    scaling = math.log2(math.e) / math.sqrt(DH)
    ahead = lax.rem(rep + shift, reps)
    behind = lax.rem(rep + reps - shift, reps)
    mate = me + 1 - 2 * lax.rem(me, 2)

    def to_tp(src, dst, snd, rcv, t):
        return pltpu.make_async_remote_copy(
            src_ref=src, dst_ref=dst, send_sem=snd, recv_sem=rcv,
            device_id=(rep, t), device_id_type=MESH,
        )

    def to_rep(src, dst, snd, rcv, r):
        return pltpu.make_async_remote_copy(
            src_ref=src, dst_ref=dst, send_sem=snd, recv_sem=rcv,
            device_id=(r, me), device_id_type=MESH,
        )

    columns = pl.ds(0, width)
    load_q = pltpu.make_async_copy(q_h, qall.at[me], loc_sem.at[0])
    load_k = pltpu.make_async_copy(kp_h, kbuf.at[:, :, columns], loc_sem.at[1])
    load_v = pltpu.make_async_copy(vp_h, vbuf.at[:, :, columns], loc_sem.at[2])
    load_nk = pltpu.make_async_copy(nk_h, nkb.at[lax.rem(me, 2)], loc_sem.at[3])
    load_nv = pltpu.make_async_copy(nv_h, nvb.at[lax.rem(me, 2)], loc_sem.at[4])
    load_slot = pltpu.make_async_copy(slot_h, slot_s, loc_sem.at[5])
    load_pt = pltpu.make_async_copy(pt_h, pt_s, loc_sem.at[6])
    load_len = pltpu.make_async_copy(len_h, len_s, loc_sem.at[7])
    load_ptv = pltpu.make_async_copy(pt_h, pt_v, loc_sem.at[8])
    load_q.start()
    load_slot.start()

    others = [ahead, behind]
    routes = plan(shift)
    around = reps // 2

    def beside(r, step):
        spot = lax.rem(r, around)
        return r - spot + lax.rem(spot + 2 * step + around, around)

    for step, _, _ in routes:
        client = beside(rep, -step)
        others += [
            beside(rep, step), client, lax.rem(client + shift, reps), beside(behind, step)
        ]

    barrier = pltpu.get_barrier_semaphore()

    def group_at(k):
        odd = lax.rem(k, 2)
        off = KVH // 2 + (1 - odd) * (k // 2) - odd * ((k + 1) // 2)
        return lax.rem(my_group + off, KVH)

    def to_peers(act):
        def of_group(k, _):
            for j in range(per_group):
                t = group_at(k) * per_group + j

                @pl.when(t != me)
                def _():
                    act(t)

            return 0

        lax.fori_loop(0, KVH, of_group, 0)

    def greet(t):
        pl.semaphore_signal(barrier, inc=1, device_id=(rep, t), device_id_type=MESH)

    to_peers(greet)
    for r in others:
        pl.semaphore_signal(barrier, inc=1, device_id=(r, me), device_id_type=MESH)
    load_pt.start()
    load_nk.start()
    load_nv.start()
    load_k.start()
    load_v.start()
    load_len.start()
    load_ptv.start()
    load_slot.wait()

    leaving = slot_s[rep]
    slot_ids = lax.broadcasted_iota(jnp.int32, (slots, DH), 0)
    lane_ids = lax.broadcasted_iota(jnp.int32, (slots, DH), 1)
    is_moving = slot_ids == leaving

    load_q.wait()
    for h in range(heads):
        part = qall[me, :, h * DH : (h + 1) * DH].astype(f32)
        qsel[:, h * DH : (h + 1) * DH] = jnp.sum(
            jnp.where(is_moving, part, 0.0), axis=0, keepdims=True
        )
    pl.semaphore_wait(barrier, tps - 1 + len(others))

    ask = to_rep(qsel, qmv.at[me], x_snd.at[0], x_rcv.at[0], behind)
    ask.start()
    to_peers(lambda t: to_tp(qall.at[me], qall.at[me], q_snd, q_rcv, t).start())
    half = lax.rem(me, 2)
    give_nk = to_tp(nkb.at[half], nkb.at[half], n_snd.at[0], n_rcv.at[0], mate)
    give_nv = to_tp(nvb.at[half], nvb.at[half], n_snd.at[1], n_rcv.at[1], mate)
    load_nk.wait()
    load_nv.wait()
    give_nk.start()
    give_nv.start()
    load_pt.wait()
    for load, buf, base in ((load_k, kbuf, 0), (load_v, vbuf, pages_most)):
        load.wait()

        def take(j, _):
            page = pt_s[leaving, j]
            rows_in = buf[jnp.maximum(page, 0), :, 0:width]
            pbuf[base + j] = jnp.where(page >= 0, rows_in, jnp.zeros((), bf16))
            return 0

        lax.fori_loop(0, pages_most, take, 0)

    ask.wait_recv()

    to_peers(lambda t: to_tp(qmv.at[me], qmv.at[me], mq_snd, mq_rcv, t).start())

    def landing(first, count):
        out = mk_ref if first < pages_most else mv_ref
        return out.at[pl.ds(first % pages_most, count)]

    taken = {p for _, first, count in routes for p in range(first, first + count)}
    moves = []
    for base in (0, pages_most):
        count = sum(base + p not in taken for p in range(pages_most))
        if count:
            moves.append(to_rep(
                pbuf.at[pl.ds(base, count)], landing(base, count),
                p_snd.at[len(moves)], p_rcv.at[len(moves)], ahead,
            ))
    legs, nexts = [], []
    for part in range(CHUNKS):
        for step, first, count in routes:
            size = count // CHUNKS
            at, n = first + part * size, len(legs)
            client_to = lax.rem(beside(rep, -step) + shift, reps)
            here = hold.at[pl.ds(at, size)]
            mine = pbuf.at[pl.ds(at, size)]
            legs.append(to_rep(mine, here, h_snd.at[n], h_rcv.at[n], beside(rep, step)))
            nexts.append(to_rep(here, landing(at, size), f_snd.at[n], f_rcv.at[n], client_to))
    for leg in legs:
        leg.start()
    for move in moves:
        move.start()

    def pass_on(*which):
        for n in which:
            if n < len(legs):
                legs[n].wait_recv()
                nexts[n].start()

    load_len.wait()
    load_ptv.wait()

    lens = jnp.zeros((slots, DH), jnp.int32)
    for i in range(slots):
        lens = jnp.where(slot_ids == i, len_s[rep * slots + i], lens)
    table = pt_v[...]
    for b in range(tokens // DH):
        token = lane_ids + b * DH
        page_of = lax.shift_right_logical(token, 3)
        left = jnp.zeros((slots, DH), jnp.int32)
        for j in range(pages_most):
            left = jnp.where(table[:, j : j + 1] == page_of, lens - j * PAGE, left)
        row = jnp.bitwise_and(token, rows - 1) + me * rows
        lim_ref[:, b * DH : (b + 1) * DH] = jnp.where(left > row, 1.0, 0.0)

    rest = pl.ds(0, tps - 1)
    all_q = to_tp(qall.at[rest], qall.at[rest], q_snd, q_rcv, mate)
    all_mq = to_tp(qmv.at[rest], qmv.at[rest], mq_snd, mq_rcv, mate)
    all_o = to_tp(osend.at[rest], orecv.at[rest], o_snd, o_rcv, mate)
    all_s = to_tp(ssend.at[rest], srecv.at[rest], s_snd, s_rcv, mate)
    all_q.wait_recv()
    if len(routes) > 1:
        pass_on(0)
        if routes[1][0] ** 2 == 1:
            pass_on(1)
    all_mq.wait_recv()

    def send_parts(k):
        for j in range(per_group):
            t = group_at(k) * per_group + j

            @pl.when(t != me)
            def _():
                to_tp(osend.at[t], orecv.at[me], o_snd, o_rcv, t).start()
                to_tp(ssend.at[t], srecv.at[me], s_snd, s_rcv, t).start()

    def attend(k):
        g = group_at(k)
        pieces = []
        for j in range(per_group):
            t = g * per_group + j
            for h in range(heads):
                own = qall[t, :, h * DH : (h + 1) * DH].astype(f32)
                moved = qmv[t, :, h * DH : (h + 1) * DH]
                pieces.append(jnp.where(is_moving, jnp.broadcast_to(moved, own.shape), own))
        query = jnp.concatenate(pieces, axis=0).astype(bf16)
        col = pl.multiple_of(g * DH, DH)
        keys = kbuf[:, :, pl.ds(col, DH)].reshape(tokens, DH)
        values = vbuf[:, :, pl.ds(col, DH)].reshape(tokens, DH)
        s = lax.dot_general(
            query, keys, (((1,), (1,)), ((), ())), preferred_element_type=f32
        ).reshape(GROUP, slots, tokens)
        s = jnp.where((lim_ref[...] > 0.5)[None], s * scaling, NEG)
        m = jnp.maximum(jnp.max(s, axis=-1, keepdims=True), LOW)
        p = jnp.exp2(s - m)
        total = jnp.sum(p, axis=-1, keepdims=True)
        o = lax.dot_general(
            p.reshape(GROUP * slots, tokens).astype(bf16), values,
            (((1,), (0,)), ((), ())), preferred_element_type=f32,
        )
        for j in range(per_group):
            t = g * per_group + j
            osend[t] = o[j * heads * slots : (j + 1) * heads * slots].astype(bf16)
            stats = jnp.zeros((slots, DH), f32)
            for h in range(heads):
                stats = jnp.where(lane_ids == slot_ids * 8 + h, m[j * heads + h], stats)
                stats = jnp.where(
                    lane_ids == slot_ids * 8 + h + DH // 2, total[j * heads + h], stats
                )
            ssend[t] = jnp.sum(stats, axis=0, keepdims=True)

    def attend_some(i, _):
        @pl.when(i > 0)
        def _():
            for j in range(UNROLL):
                send_parts((i - 1) * UNROLL + j)

        for j in range(UNROLL):
            attend(i * UNROLL + j)
        return 0

    if len(routes) == 1:
        pass_on(0)
    elif routes and routes[1][0] ** 2 == 1:
        pass_on(2, 3)
    elif routes:
        pass_on(1, 2)
    lax.fori_loop(0, KVH // UNROLL, attend_some, 0)
    if len(routes) == 1:
        pass_on(1)
    elif routes and routes[1][0] ** 2 != 1:
        pass_on(3)
    orecv[me] = osend[me]
    srecv[me] = ssend[me]

    give_nk.wait_recv()
    give_nv.wait_recv()
    for j in range(UNROLL):
        send_parts(KVH - UNROLL + j)
    at_row = lax.broadcasted_iota(jnp.int32, (DH // 2, DH), 0)
    at_col = lax.broadcasted_iota(jnp.int32, (DH // 2, DH), 1)
    fresh = []
    for buf in (nkb, nvb):
        both = jnp.zeros((slots, DH), f32)
        for i in range(2):
            place = jnp.where(at_col == at_row + i * (DH // 2), 1.0, 0.0).astype(bf16)
            both = both + jnp.dot(buf[i], place, preferred_element_type=f32)
        fresh.append(both)
    new_key, new_value = fresh
    new_scores = []
    for h in range(heads):
        own = qall[me, :, h * DH : (h + 1) * DH].astype(f32)
        new_scores.append(jnp.sum(own * new_key, axis=-1, keepdims=True) * scaling)

    all_o.wait_recv()
    all_s.wait_recv()

    stats = jnp.concatenate([srecv[t] for t in range(tps)], axis=0)
    peaks = jnp.max(stats, axis=0, keepdims=True)
    factors = jnp.exp2(stats - peaks)
    totals = jnp.sum(factors * pltpu.roll(stats, DH // 2, 1), axis=0, keepdims=True)

    def column(line, h):
        spread = jnp.where(lane_ids == slot_ids * 8 + h, line, 0.0)
        return jnp.sum(spread, axis=-1, keepdims=True)

    mixed = [jnp.zeros((slots, DH), f32) for _ in range(heads)]
    for t in range(tps):
        part = orecv[t].astype(f32)
        for h in range(heads):
            mixed[h] = mixed[h] + column(factors[t : t + 1], h) * part[h * slots : (h + 1) * slots]
    peak = [column(peaks, h) for h in range(heads)]
    total = [column(totals, h) for h in range(heads)]

    for h in range(heads):
        rsend[h] = jnp.sum(jnp.where(is_moving, mixed[h], 0.0), axis=0, keepdims=True)
    for at, columns_of in ((heads, peak), (heads + 1, total)):
        line = jnp.zeros((slots, DH), f32)
        for h in range(heads):
            line = jnp.where(lane_ids == h, columns_of[h], line)
        rsend[at] = jnp.sum(jnp.where(is_moving, line, 0.0), axis=0, keepdims=True)
    answer = to_rep(rsend, rrecv, x_snd.at[1], x_rcv.at[1], ahead)
    answer.start()
    answer.wait_recv()
    moving = is_moving[:, 0:1]
    for h in range(heads):
        mix = jnp.where(is_moving, jnp.broadcast_to(rrecv[h], (slots, DH)), mixed[h])
        old_peak = jnp.where(moving, rrecv[heads][:, h : h + 1], peak[h])
        old_total = jnp.where(moving, rrecv[heads + 1][:, h : h + 1], total[h])
        new_score = new_scores[h]
        top = jnp.maximum(old_peak, new_score)
        old_scale = jnp.exp2(old_peak - top)
        new_weight = jnp.exp2(new_score - top)
        denominator = old_total * old_scale + new_weight
        rounded = new_weight.astype(bf16).astype(f32)
        out = (mix * old_scale + rounded * new_value) / denominator
        att_ref[:, h * DH : (h + 1) * DH] = out.astype(bf16)

    ask.wait_send()
    answer.wait_send()
    give_nk.wait_send()
    give_nv.wait_send()

    for sends in (all_q, all_mq, all_o, all_s):
        sends.wait_send()
    for leg, after in zip(legs, nexts):
        leg.wait_send()
        after.wait()
    for move in moves:
        move.wait()


def call_for(shift, requests, replicas, tps, slots, pages_most, pool, rows, width, columns):
    f32, bf16 = jnp.float32, jnp.bfloat16
    heads = H // tps
    vmem = pl.BlockSpec(memory_space=pltpu.VMEM)
    hbm = pl.BlockSpec(memory_space=pl.ANY)
    dma = pltpu.SemaphoreType.DMA
    moved = jax.ShapeDtypeStruct((pages_most, rows, width), bf16)
    return pl.pallas_call(
        functools.partial(kernel, shift),
        out_shape=(jax.ShapeDtypeStruct((slots, columns), bf16), moved, moved),
        in_specs=[hbm] * 8,
        out_specs=(vmem, hbm, hbm),
        scratch_shapes=[
            pltpu.SMEM((requests,), jnp.int32),
            pltpu.SMEM((slots, pages_most), jnp.int32),
            pltpu.SMEM((replicas,), jnp.int32),
            pltpu.VMEM((slots, pages_most), jnp.int32),
            pltpu.VMEM((pool, rows, width + DH), bf16),
            pltpu.VMEM((pool, rows, width + DH), bf16),
            pltpu.VMEM((tps, slots, columns), bf16),
            pltpu.VMEM((tps, 1, columns), f32),
            pltpu.VMEM((1, columns), f32),
            pltpu.VMEM((2, slots, DH // 2), bf16),
            pltpu.VMEM((2, slots, DH // 2), bf16),
            pltpu.VMEM((2 * pages_most, rows, width), bf16),
            pltpu.VMEM((slots, pool * rows), f32),
            pltpu.VMEM((tps, heads * slots, DH), bf16),
            pltpu.VMEM((tps, heads * slots, DH), bf16),
            pltpu.VMEM((tps, 1, DH), f32),
            pltpu.VMEM((tps, 1, DH), f32),
            pltpu.VMEM((heads + 2, 1, DH), f32),
            pltpu.VMEM((heads + 2, 1, DH), f32),
            pltpu.VMEM((2 * pages_most, rows, width), bf16),
            dma((9,)),
            dma, dma,
            dma, dma,
            dma((2,)), dma((2,)),
            dma, dma,
            dma, dma,
            dma((2,)), dma((2,)),
            dma((2,)), dma((2,)),
            dma((2 * CHUNKS,)), dma((2 * CHUNKS,)),
            dma((2 * CHUNKS,)), dma((2 * CHUNKS,)),
        ],
        compiler_params=pltpu.CompilerParams(
            collective_id=shift, has_side_effects=True,
        ),
        name="serve_%d" % shift,
    )


ONLY = None


def body(
    queries, new_keys, new_values, key_pool, value_pool, lengths, page_table, mig_slot, mig_dst
):
    replicas, tps = lax.axis_size("rep"), lax.axis_size("tp")
    slots, pages_most = page_table.shape
    sizes = (lengths.size, mig_slot.size, tps, slots, pages_most, *key_pool.shape, queries.shape[1])
    operands = (
        lengths, page_table, mig_slot,
        queries, new_keys, new_values, key_pool, value_pool,
    )
    if ONLY is not None:
        made = call_for(ONLY, *sizes)(*operands)
    else:
        made = lax.switch(
            mig_dst[0] - 1,
            [call_for(shift, *sizes) for shift in range(1, replicas)],
            *operands,
        )
    return pl.pallas_call(
        finish,
        out_shape=tuple(jax.ShapeDtypeStruct(a.shape, a.dtype) for a in made),
        in_specs=[pl.BlockSpec(memory_space=pl.ANY)] * 3,
        out_specs=(pl.BlockSpec(memory_space=pl.ANY),) * 3,
        scratch_shapes=[pltpu.SemaphoreType.DMA((3,))],
        name="finish",
    )(*made)


def solution(mesh):
    placed = (
        P("rep", "tp"),
        P("rep", "tp"),
        P("rep", "tp"),
        P("rep", "tp", None),
        P("rep", "tp", None),
        P(),
        P("rep", None),
        P(),
        P(),
    )
    return jax.shard_map(
        body,
        mesh=mesh,
        in_specs=placed,
        out_specs=(P("rep", "tp"), P("rep", "tp", None), P("rep", "tp", None)),
        check_vma=False,
    )
```

```python
import functools
import math

import jax
import jax.numpy as jnp
from jax import lax
from jax.experimental import pallas as pl
from jax.experimental.pallas import tpu as pltpu
from jax.sharding import PartitionSpec as P

H = 64
KVH = 8
DH = 128
PAGE = 128
GROUP = H // KVH
NEG = -1e30
LOW = -1e29
UNROLL = 2
MESH = pl.DeviceIdType.MESH
CHUNKS = 2


def plan(shift):
    return {
        5: ((-3, 18, 6),),
        6: ((-2, 16, 8),),
        7: ((1, 0, 12), (-2, 12, 12)),
        8: ((1, 0, 12), (-1, 12, 12)),
        9: ((-1, 0, 12), (2, 12, 12)),
        10: ((2, 16, 8),),
        11: ((3, 18, 6),),
    }.get(shift % 16, ())


EARLY = {4: 2, 5: 1, 7: 1, 8: 1, 9: 1, 10: 2, 11: 1, 12: 2, 20: 2, 23: 1, 24: 1, 25: 1, 26: 2, 28: 2}


def finish(att, mk, mv, att_out, mk_out, mv_out, sem):
    copies = [
        pltpu.make_async_copy(src, dst, sem.at[i])
        for i, (src, dst) in enumerate(((mk, mk_out), (mv, mv_out), (att, att_out)))
    ]
    for copy in copies:
        copy.start()
    for copy in copies:
        copy.wait()


def kernel(
    shift,
    len_h, pt_h, slot_h, q_h, nk_h, nv_h, kp_h, vp_h,
    att_ref, mk_ref, mv_ref,
    len_s, pt_s, slot_s, pt_v, kbuf, vbuf, qall, qmv, qsel, nkb, nvb, pbuf, lim_ref,
    osend, orecv, ssend, srecv, rsend, rrecv, hold,
    loc_sem, q_snd, q_rcv, mq_snd, mq_rcv, n_snd, n_rcv, o_snd, o_rcv, s_snd, s_rcv,
    p_snd, p_rcv, x_snd, x_rcv, h_snd, h_rcv, f_snd, f_rcv,
):
    f32, bf16 = jnp.float32, jnp.bfloat16
    reps, tps = lax.axis_size("rep"), lax.axis_size("tp")
    rep, me = lax.axis_index("rep"), lax.axis_index("tp")
    slots, pages_most = pt_s.shape
    pool, rows, width = kp_h.shape
    tokens = pool * rows
    heads = H // tps
    per_group = tps // KVH
    my_group = me // per_group
    scaling = math.log2(math.e) / math.sqrt(DH)
    ahead = lax.rem(rep + shift, reps)
    behind = lax.rem(rep + reps - shift, reps)
    mate = me + 1 - 2 * lax.rem(me, 2)

    def to_tp(src, dst, snd, rcv, t):
        return pltpu.make_async_remote_copy(
            src_ref=src, dst_ref=dst, send_sem=snd, recv_sem=rcv,
            device_id=(rep, t), device_id_type=MESH,
        )

    def to_rep(src, dst, snd, rcv, r):
        return pltpu.make_async_remote_copy(
            src_ref=src, dst_ref=dst, send_sem=snd, recv_sem=rcv,
            device_id=(r, me), device_id_type=MESH,
        )

    columns = pl.ds(0, width)
    load_q = pltpu.make_async_copy(q_h, qall.at[me], loc_sem.at[0])
    load_k = pltpu.make_async_copy(kp_h, kbuf.at[:, :, columns], loc_sem.at[1])
    load_v = pltpu.make_async_copy(vp_h, vbuf.at[:, :, columns], loc_sem.at[2])
    load_nk = pltpu.make_async_copy(nk_h, nkb.at[lax.rem(me, 2)], loc_sem.at[3])
    load_nv = pltpu.make_async_copy(nv_h, nvb.at[lax.rem(me, 2)], loc_sem.at[4])
    load_slot = pltpu.make_async_copy(slot_h, slot_s, loc_sem.at[5])
    load_pt = pltpu.make_async_copy(pt_h, pt_s, loc_sem.at[6])
    load_len = pltpu.make_async_copy(len_h, len_s, loc_sem.at[7])
    load_ptv = pltpu.make_async_copy(pt_h, pt_v, loc_sem.at[8])
    load_q.start()
    load_slot.start()

    others = [ahead, behind]
    routes = plan(shift)
    around = reps // 2

    def beside(r, step):
        spot = lax.rem(r, around)
        return r - spot + lax.rem(spot + 2 * step + around, around)

    for step, _, _ in routes:
        client = beside(rep, -step)
        others += [
            beside(rep, step), client, lax.rem(client + shift, reps), beside(behind, step)
        ]

    barrier = pltpu.get_barrier_semaphore()

    def group_at(k):
        odd = lax.rem(k, 2)
        off = KVH // 2 + (1 - odd) * (k // 2) - odd * ((k + 1) // 2)
        return lax.rem(my_group + off, KVH)

    def to_peers(act):
        def of_group(k, _):
            for j in range(per_group):
                t = group_at(k) * per_group + j

                @pl.when(t != me)
                def _():
                    act(t)

            return 0

        lax.fori_loop(0, KVH, of_group, 0)

    def greet(t):
        pl.semaphore_signal(barrier, inc=1, device_id=(rep, t), device_id_type=MESH)

    to_peers(greet)
    for r in others:
        pl.semaphore_signal(barrier, inc=1, device_id=(r, me), device_id_type=MESH)
    load_pt.start()
    load_nk.start()
    load_nv.start()
    load_k.start()
    load_v.start()
    load_len.start()
    load_ptv.start()
    load_slot.wait()

    leaving = slot_s[rep]
    slot_ids = lax.broadcasted_iota(jnp.int32, (slots, DH), 0)
    lane_ids = lax.broadcasted_iota(jnp.int32, (slots, DH), 1)
    is_moving = slot_ids == leaving

    load_q.wait()
    for h in range(heads):
        part = qall[me, :, h * DH : (h + 1) * DH].astype(f32)
        qsel[:, h * DH : (h + 1) * DH] = jnp.sum(
            jnp.where(is_moving, part, 0.0), axis=0, keepdims=True
        )
    pl.semaphore_wait(barrier, tps - 1 + len(others))

    ask = to_rep(qsel, qmv.at[me], x_snd.at[0], x_rcv.at[0], behind)
    ask.start()
    to_peers(lambda t: to_tp(qall.at[me], qall.at[me], q_snd, q_rcv, t).start())
    half = lax.rem(me, 2)
    give_nk = to_tp(nkb.at[half], nkb.at[half], n_snd.at[0], n_rcv.at[0], mate)
    give_nv = to_tp(nvb.at[half], nvb.at[half], n_snd.at[1], n_rcv.at[1], mate)
    load_nk.wait()
    load_nv.wait()
    give_nk.start()
    give_nv.start()
    load_pt.wait()
    for load, buf, base in ((load_k, kbuf, 0), (load_v, vbuf, pages_most)):
        load.wait()

        def take(j, _):
            page = pt_s[leaving, j]
            rows_in = buf[jnp.maximum(page, 0), :, 0:width]
            pbuf[base + j] = jnp.where(page >= 0, rows_in, jnp.zeros((), bf16))
            return 0

        lax.fori_loop(0, pages_most, take, 0)

    def landing(first, count):
        out = mk_ref if first < pages_most else mv_ref
        return out.at[pl.ds(first % pages_most, count)]

    taken = {p for _, first, count in routes for p in range(first, first + count)}
    moves = []
    for base in (0, pages_most):
        count = sum(base + p not in taken for p in range(pages_most))
        if count:
            moves.append(to_rep(
                pbuf.at[pl.ds(base, count)], landing(base, count),
                p_snd.at[len(moves)], p_rcv.at[len(moves)], ahead,
            ))
    legs, nexts = [], []
    for part in range(CHUNKS):
        for step, first, count in routes:
            size = count // CHUNKS
            at, n = first + part * size, len(legs)
            client_to = lax.rem(beside(rep, -step) + shift, reps)
            here = hold.at[pl.ds(at, size)]
            mine = pbuf.at[pl.ds(at, size)]
            legs.append(to_rep(mine, here, h_snd.at[n], h_rcv.at[n], beside(rep, step)))
            nexts.append(to_rep(here, landing(at, size), f_snd.at[n], f_rcv.at[n], client_to))
    early = EARLY.get(shift, 0)
    if early > 0:
        for copy in legs + (moves if early > 1 else []):
            copy.start()
    ask.wait_recv()

    to_peers(lambda t: to_tp(qmv.at[me], qmv.at[me], mq_snd, mq_rcv, t).start())
    for copy in (legs if early < 1 else []) + (moves if early < 2 else []):
        copy.start()

    def pass_on(*which):
        for n in which:
            if n < len(legs):
                legs[n].wait_recv()
                nexts[n].start()

    load_len.wait()
    load_ptv.wait()

    lens = jnp.zeros((slots, DH), jnp.int32)
    for i in range(slots):
        lens = jnp.where(slot_ids == i, len_s[rep * slots + i], lens)
    table = pt_v[...]
    for b in range(tokens // DH):
        token = lane_ids + b * DH
        page_of = lax.shift_right_logical(token, 3)
        left = jnp.zeros((slots, DH), jnp.int32)
        for j in range(pages_most):
            left = jnp.where(table[:, j : j + 1] == page_of, lens - j * PAGE, left)
        row = jnp.bitwise_and(token, rows - 1) + me * rows
        lim_ref[:, b * DH : (b + 1) * DH] = jnp.where(left > row, 1.0, 0.0)

    rest = pl.ds(0, tps - 1)
    all_q = to_tp(qall.at[rest], qall.at[rest], q_snd, q_rcv, mate)
    all_mq = to_tp(qmv.at[rest], qmv.at[rest], mq_snd, mq_rcv, mate)
    all_o = to_tp(osend.at[rest], orecv.at[rest], o_snd, o_rcv, mate)
    all_s = to_tp(ssend.at[rest], srecv.at[rest], s_snd, s_rcv, mate)
    all_q.wait_recv()
    if len(routes) > 1:
        pass_on(0)
        if routes[1][0] ** 2 == 1:
            pass_on(1)
    all_mq.wait_recv()

    def send_parts(k):
        for j in range(per_group):
            t = group_at(k) * per_group + j

            @pl.when(t != me)
            def _():
                to_tp(osend.at[t], orecv.at[me], o_snd, o_rcv, t).start()
                to_tp(ssend.at[t], srecv.at[me], s_snd, s_rcv, t).start()

    def attend(k):
        g = group_at(k)
        pieces = []
        for j in range(per_group):
            t = g * per_group + j
            for h in range(heads):
                own = qall[t, :, h * DH : (h + 1) * DH].astype(f32)
                moved = qmv[t, :, h * DH : (h + 1) * DH]
                pieces.append(jnp.where(is_moving, jnp.broadcast_to(moved, own.shape), own))
        query = jnp.concatenate(pieces, axis=0).astype(bf16)
        col = pl.multiple_of(g * DH, DH)
        keys = kbuf[:, :, pl.ds(col, DH)].reshape(tokens, DH)
        values = vbuf[:, :, pl.ds(col, DH)].reshape(tokens, DH)
        s = lax.dot_general(
            query, keys, (((1,), (1,)), ((), ())), preferred_element_type=f32
        ).reshape(GROUP, slots, tokens)
        s = jnp.where((lim_ref[...] > 0.5)[None], s * scaling, NEG)
        m = jnp.maximum(jnp.max(s, axis=-1, keepdims=True), LOW)
        p = jnp.exp2(s - m)
        total = jnp.sum(p, axis=-1, keepdims=True)
        o = lax.dot_general(
            p.reshape(GROUP * slots, tokens).astype(bf16), values,
            (((1,), (0,)), ((), ())), preferred_element_type=f32,
        )
        for j in range(per_group):
            t = g * per_group + j
            osend[t] = o[j * heads * slots : (j + 1) * heads * slots].astype(bf16)
            stats = jnp.zeros((slots, DH), f32)
            for h in range(heads):
                stats = jnp.where(lane_ids == slot_ids * 8 + h, m[j * heads + h], stats)
                stats = jnp.where(
                    lane_ids == slot_ids * 8 + h + DH // 2, total[j * heads + h], stats
                )
            ssend[t] = jnp.sum(stats, axis=0, keepdims=True)

    def attend_some(i, _):
        @pl.when(i > 0)
        def _():
            for j in range(UNROLL):
                send_parts((i - 1) * UNROLL + j)

        for j in range(UNROLL):
            attend(i * UNROLL + j)
        return 0

    if len(routes) == 1:
        pass_on(0)
    elif routes and routes[1][0] ** 2 == 1:
        pass_on(2, 3)
    elif routes:
        pass_on(1, 2)
    lax.fori_loop(0, KVH // UNROLL, attend_some, 0)
    if len(routes) == 1:
        pass_on(1)
    elif routes and routes[1][0] ** 2 != 1:
        pass_on(3)
    orecv[me] = osend[me]
    srecv[me] = ssend[me]

    give_nk.wait_recv()
    give_nv.wait_recv()
    for j in range(UNROLL):
        send_parts(KVH - UNROLL + j)
    at_row = lax.broadcasted_iota(jnp.int32, (DH // 2, DH), 0)
    at_col = lax.broadcasted_iota(jnp.int32, (DH // 2, DH), 1)
    fresh = []
    for buf in (nkb, nvb):
        both = jnp.zeros((slots, DH), f32)
        for i in range(2):
            place = jnp.where(at_col == at_row + i * (DH // 2), 1.0, 0.0).astype(bf16)
            both = both + jnp.dot(buf[i], place, preferred_element_type=f32)
        fresh.append(both)
    new_key, new_value = fresh
    new_scores = []
    for h in range(heads):
        own = qall[me, :, h * DH : (h + 1) * DH].astype(f32)
        new_scores.append(jnp.sum(own * new_key, axis=-1, keepdims=True) * scaling)

    all_o.wait_recv()
    all_s.wait_recv()

    stats = jnp.concatenate([srecv[t] for t in range(tps)], axis=0)
    peaks = jnp.max(stats, axis=0, keepdims=True)
    factors = jnp.exp2(stats - peaks)
    totals = jnp.sum(factors * pltpu.roll(stats, DH // 2, 1), axis=0, keepdims=True)

    def column(line, h):
        spread = jnp.where(lane_ids == slot_ids * 8 + h, line, 0.0)
        return jnp.sum(spread, axis=-1, keepdims=True)

    mixed = [jnp.zeros((slots, DH), f32) for _ in range(heads)]
    for t in range(tps):
        part = orecv[t].astype(f32)
        for h in range(heads):
            mixed[h] = mixed[h] + column(factors[t : t + 1], h) * part[h * slots : (h + 1) * slots]
    peak = [column(peaks, h) for h in range(heads)]
    total = [column(totals, h) for h in range(heads)]

    for h in range(heads):
        rsend[h] = jnp.sum(jnp.where(is_moving, mixed[h], 0.0), axis=0, keepdims=True)
    for at, columns_of in ((heads, peak), (heads + 1, total)):
        line = jnp.zeros((slots, DH), f32)
        for h in range(heads):
            line = jnp.where(lane_ids == h, columns_of[h], line)
        rsend[at] = jnp.sum(jnp.where(is_moving, line, 0.0), axis=0, keepdims=True)
    answer = to_rep(rsend, rrecv, x_snd.at[1], x_rcv.at[1], ahead)
    answer.start()
    answer.wait_recv()
    moving = is_moving[:, 0:1]
    for h in range(heads):
        mix = jnp.where(is_moving, jnp.broadcast_to(rrecv[h], (slots, DH)), mixed[h])
        old_peak = jnp.where(moving, rrecv[heads][:, h : h + 1], peak[h])
        old_total = jnp.where(moving, rrecv[heads + 1][:, h : h + 1], total[h])
        new_score = new_scores[h]
        top = jnp.maximum(old_peak, new_score)
        old_scale = jnp.exp2(old_peak - top)
        new_weight = jnp.exp2(new_score - top)
        denominator = old_total * old_scale + new_weight
        rounded = new_weight.astype(bf16).astype(f32)
        out = (mix * old_scale + rounded * new_value) / denominator
        att_ref[:, h * DH : (h + 1) * DH] = out.astype(bf16)

    ask.wait_send()
    answer.wait_send()
    give_nk.wait_send()
    give_nv.wait_send()

    for sends in (all_q, all_mq, all_o, all_s):
        sends.wait_send()
    for leg, after in zip(legs, nexts):
        leg.wait_send()
        after.wait()
    for move in moves:
        move.wait()


def call_for(shift, requests, replicas, tps, slots, pages_most, pool, rows, width, columns):
    f32, bf16 = jnp.float32, jnp.bfloat16
    heads = H // tps
    vmem = pl.BlockSpec(memory_space=pltpu.VMEM)
    hbm = pl.BlockSpec(memory_space=pl.ANY)
    dma = pltpu.SemaphoreType.DMA
    moved = jax.ShapeDtypeStruct((pages_most, rows, width), bf16)
    return pl.pallas_call(
        functools.partial(kernel, shift),
        out_shape=(jax.ShapeDtypeStruct((slots, columns), bf16), moved, moved),
        in_specs=[hbm] * 8,
        out_specs=(vmem, hbm, hbm),
        scratch_shapes=[
            pltpu.SMEM((requests,), jnp.int32),
            pltpu.SMEM((slots, pages_most), jnp.int32),
            pltpu.SMEM((replicas,), jnp.int32),
            pltpu.VMEM((slots, pages_most), jnp.int32),
            pltpu.VMEM((pool, rows, width + DH), bf16),
            pltpu.VMEM((pool, rows, width + DH), bf16),
            pltpu.VMEM((tps, slots, columns), bf16),
            pltpu.VMEM((tps, 1, columns), f32),
            pltpu.VMEM((1, columns), f32),
            pltpu.VMEM((2, slots, DH // 2), bf16),
            pltpu.VMEM((2, slots, DH // 2), bf16),
            pltpu.VMEM((2 * pages_most, rows, width), bf16),
            pltpu.VMEM((slots, pool * rows), f32),
            pltpu.VMEM((tps, heads * slots, DH), bf16),
            pltpu.VMEM((tps, heads * slots, DH), bf16),
            pltpu.VMEM((tps, 1, DH), f32),
            pltpu.VMEM((tps, 1, DH), f32),
            pltpu.VMEM((heads + 2, 1, DH), f32),
            pltpu.VMEM((heads + 2, 1, DH), f32),
            pltpu.VMEM((2 * pages_most, rows, width), bf16),
            dma((9,)),
            dma, dma,
            dma, dma,
            dma((2,)), dma((2,)),
            dma, dma,
            dma, dma,
            dma((2,)), dma((2,)),
            dma((2,)), dma((2,)),
            dma((2 * CHUNKS,)), dma((2 * CHUNKS,)),
            dma((2 * CHUNKS,)), dma((2 * CHUNKS,)),
        ],
        compiler_params=pltpu.CompilerParams(
            collective_id=shift, has_side_effects=True,
        ),
        name="serve_%d" % shift,
    )


ONLY = None


def body(
    queries, new_keys, new_values, key_pool, value_pool, lengths, page_table, mig_slot, mig_dst
):
    replicas, tps = lax.axis_size("rep"), lax.axis_size("tp")
    slots, pages_most = page_table.shape
    sizes = (lengths.size, mig_slot.size, tps, slots, pages_most, *key_pool.shape, queries.shape[1])
    operands = (
        lengths, page_table, mig_slot,
        queries, new_keys, new_values, key_pool, value_pool,
    )
    if ONLY is not None:
        made = call_for(ONLY, *sizes)(*operands)
    else:
        made = lax.switch(
            mig_dst[0] - 1,
            [call_for(shift, *sizes) for shift in range(1, replicas)],
            *operands,
        )
    return pl.pallas_call(
        finish,
        out_shape=tuple(jax.ShapeDtypeStruct(a.shape, a.dtype) for a in made),
        in_specs=[pl.BlockSpec(memory_space=pl.ANY)] * 3,
        out_specs=(pl.BlockSpec(memory_space=pl.ANY),) * 3,
        scratch_shapes=[pltpu.SemaphoreType.DMA((3,))],
        name="finish",
    )(*made)


def solution(mesh):
    placed = (
        P("rep", "tp"),
        P("rep", "tp"),
        P("rep", "tp"),
        P("rep", "tp", None),
        P("rep", "tp", None),
        P(),
        P("rep", None),
        P(),
        P(),
    )
    return jax.shard_map(
        body,
        mesh=mesh,
        in_specs=placed,
        out_specs=(P("rep", "tp"), P("rep", "tp", None), P("rep", "tp", None)),
        check_vma=False,
    )
```
